32 devices in a mesh: dp: 4 (over x, core), fsdp: 2 (over y), tensor: 4 (over z).
Axes of the slice: x: 2, y: 2, z: 4, core: 2. Of those that a mesh axis runs over, the one named last changes fastest.
Arguments:
- tokens: bfloat16 [8, 768, 8192], P(('dp', 'fsdp'), 'tensor'), may hold values from -6 to 6
- norm_gain: float32 [8192], replicated, may hold values from 0.85 to 4
- w_qkv: bfloat16 [8192, 5120], P(('dp', 'fsdp'), 'tensor'), may hold values from -0.3 to 0.3
- a_query: bfloat16 [8192, 16], replicated, may hold values from -0.0625 to 0.0625
- query_up_adapter: bfloat16 [16, 4096], P(None, 'tensor'), may hold values from -1.5 to 1.5
- a_value: bfloat16 [8192, 16], replicated, may hold values from -0.0625 to 0.0625
- value_up_adapter: bfloat16 [16, 512], P(None, 'tensor'), may hold values from -1.5 to 1.5
- out_grad: bfloat16 [8, 768, 4096], P(('dp', 'fsdp'), 'tensor'), may hold values from -6 to 6
Outputs:
- attn_out: bfloat16 [8, 768, 4096], P(('dp', 'fsdp'), 'tensor')
- grad_a_query: float32 [8192, 16], replicated
- grad_b_query: float32 [16, 4096], P(None, 'tensor')
- grad_a_value: float32 [8192, 16], replicated
- grad_b_value: float32 [16, 512], P(None, 'tensor')
The draws below stay inside these ranges and needn't reach their ends.
All inputs are finite; a program needn't handle non-finite values.
Results may differ from the reference program's by a relative error of at most 0.015.
The reference program's roundings to bfloat16 on the way count: a program that leaves them out, or rounds other values in their place, can miss the bound.
Values may be sent and summed in bfloat16 or wider, within the bound.
A program may use at most 256 MiB of HBM per device.

```python
import math
import jax
import jax.numpy as jnp
from jax import lax

D = 8192
KV = 4
HD = 128
RANK = 16
QUERY_PER_KV = 8
SEQ = 768
BATCH = 8
QCOLS = 4096
QKV = 5120


WEIGHT_EDGE = 0.296875


def draw_norm_gain(key, part):
    return 1.0 + 0.15 * jax.random.uniform(key, (D,), jnp.float32, -1.0, 1.0)


def draw_tokens(key, part):
    base = jax.random.normal(jax.random.fold_in(key, 11), (BATCH, SEQ, D), jnp.float32)
    return jnp.clip(base, -6.0, 6.0).astype(jnp.bfloat16)


def draw_w_qkv(key, part):
    base = jax.random.normal(jax.random.fold_in(key, 21), (D, QKV), jnp.float32) * (1.0 / math.sqrt(D))
    return jnp.clip(base, -WEIGHT_EDGE, WEIGHT_EDGE).astype(jnp.bfloat16)


def steps_of(stream_key, shape, pieces, least, largest):
    gain = 1.0
    for position, parts in pieces:
        heights = jax.random.uniform(jax.random.fold_in(jax.random.fold_in(stream_key, 6), position), (parts,), jnp.float32, least / len(pieces), largest / len(pieces))
        gain = gain * jnp.repeat(jnp.exp(heights), shape[position] // parts).reshape((-1,) + (1,) * (len(shape) - 1 - position))
    return gain


def normal_values(stream_key, extent, width, bound, shards=(), kind=jnp.bfloat16):
    loudness = steps_of(stream_key, extent, shards, -0.22, 0.18) if shards else 1.0
    drawn = jax.random.normal(stream_key, extent, jnp.float32) * width * loudness
    return jnp.minimum(jnp.maximum(drawn, -bound), bound).astype(kind)


def setup_inputs(seed: int = 0) -> dict:
    keys = jax.random.split(jax.random.key(seed), 9)
    tokens = draw_tokens(jax.random.fold_in(keys[8], 71), 0)
    norm_gain = draw_norm_gain(jax.random.fold_in(keys[8], 71), 0)
    w_qkv = draw_w_qkv(jax.random.fold_in(keys[8], 71), 0)
    a_query = normal_values(keys[3], (D, RANK), D ** -0.5, 0.0625)
    query_up_adapter = normal_values(keys[4], (RANK, QCOLS), RANK ** -0.5, 1.5, ((1, 4),))
    a_value = normal_values(keys[5], (D, RANK), D ** -0.5, 0.0625)
    value_up_adapter = normal_values(keys[6], (RANK, KV * HD), RANK ** -0.5, 1.5, ((1, 4),))
    out_grad = normal_values(keys[7], (BATCH, SEQ, QCOLS), 1.0, 6.0, ((0, 8), (1, 4)))
    return {"tokens": tokens, "norm_gain": norm_gain, "w_qkv": w_qkv, "a_query": a_query, "query_up_adapter": query_up_adapter, "a_value": a_value, "value_up_adapter": value_up_adapter, "out_grad": out_grad}


EPSILON = 1e-05
ADAPTER_SCALE = 2.0
ROPE_BASE = 500000.0

def normalize(own_rows, norm_gain):
    widened = own_rows.astype(jnp.float32)
    mean_square = lax.optimization_barrier(jnp.mean(widened * widened, axis=-1, keepdims=True))
    return (widened * lax.rsqrt(mean_square + EPSILON) * norm_gain).astype(jnp.bfloat16)

def rotary(heads_block):
    sequence_length = heads_block.shape[0]
    half_dim = heads_block.shape[-1] // 2
    positions = jnp.arange(sequence_length, dtype=jnp.float32)[:, None]
    inv_freq = ROPE_BASE ** (-jnp.arange(half_dim, dtype=jnp.float32) / half_dim)
    angles = positions * inv_freq
    cosine = jnp.cos(angles)[:, None, :]
    sine_table = jnp.sin(angles)[:, None, :]
    front_half = heads_block[..., :half_dim].astype(jnp.float32)
    back_half = heads_block[..., half_dim:].astype(jnp.float32)
    turned = jnp.concatenate([front_half * cosine - back_half * sine_table, back_half * cosine + front_half * sine_table], -1)
    return turned.astype(jnp.bfloat16)

def attend(query_rows, key_heads, value_rows):
    sequence_length = query_rows.shape[0]
    kv_heads = key_heads.shape[1] // HD
    rot_queries = rotary(query_rows.reshape(sequence_length, kv_heads * QUERY_PER_KV, HD))
    rot_keys = rotary(key_heads.reshape(sequence_length, kv_heads, HD))
    split_values = value_rows.reshape(sequence_length, kv_heads, HD)
    causal = jnp.arange(sequence_length)[:, None] >= jnp.arange(sequence_length)[None, :]

    def one_head(head_index):
        q_head = lax.dynamic_index_in_dim(rot_queries, head_index, 1, keepdims=False)
        k_head = lax.dynamic_index_in_dim(rot_keys, head_index // QUERY_PER_KV, 1, keepdims=False)
        v_head = lax.dynamic_index_in_dim(split_values, head_index // QUERY_PER_KV, 1, keepdims=False)
        scores = jnp.dot(q_head, k_head.T, preferred_element_type=jnp.float32) * (1.0 / math.sqrt(HD))
        scores = jnp.where(causal, scores, -1e+30)
        row_max = lax.optimization_barrier(jnp.max(scores, axis=-1, keepdims=True))
        weights = jnp.exp(scores - row_max)
        probabilities = (weights / lax.optimization_barrier(jnp.sum(weights, axis=-1, keepdims=True))).astype(jnp.bfloat16)
        return jnp.dot(probabilities, v_head, preferred_element_type=jnp.float32).astype(jnp.bfloat16)
    per_head = lax.map(one_head, jnp.arange(kv_heads * QUERY_PER_KV, dtype=jnp.int32))
    return jnp.transpose(per_head, (1, 0, 2)).reshape(sequence_length, kv_heads * QUERY_PER_KV * HD)

def reference(tokens, norm_gain, w_qkv, a_query, query_up_adapter, a_value, value_up_adapter, out_grad):
    adapters = jnp.concatenate([a_query, a_value], 1)
    narrow_rank_rows = a_query.shape[1]

    def one_sequence(pair):
        own_rows, grad_rows = pair
        normed_input = normalize(own_rows, norm_gain)
        sequence_length = normed_input.shape[0]
        projected = jnp.dot(normed_input, w_qkv, preferred_element_type=jnp.float32)
        down_projected = jnp.dot(normed_input, adapters, preferred_element_type=jnp.float32).astype(jnp.bfloat16)
        grouped_queries = projected.reshape(sequence_length, KV, QUERY_PER_KV + 2, HD)
        query_rows = (grouped_queries[:, :, :QUERY_PER_KV].reshape(sequence_length, -1) + ADAPTER_SCALE * jnp.dot(down_projected[:, :narrow_rank_rows], query_up_adapter, preferred_element_type=jnp.float32)).astype(jnp.bfloat16)
        key_heads = grouped_queries[:, :, QUERY_PER_KV].reshape(sequence_length, -1).astype(jnp.bfloat16)
        value_rows = (grouped_queries[:, :, QUERY_PER_KV + 1].reshape(sequence_length, -1) + ADAPTER_SCALE * jnp.dot(down_projected[:, narrow_rank_rows:], value_up_adapter, preferred_element_type=jnp.float32)).astype(jnp.bfloat16)
        attended, pullback = jax.vjp(attend, query_rows, key_heads, value_rows)
        query_gradient, grad_keys, value_gradient = pullback(grad_rows)
        query_up_gradient = ADAPTER_SCALE * jnp.einsum('fb,fd->bd', down_projected[:, :narrow_rank_rows], query_gradient, preferred_element_type=jnp.float32)
        value_up_gradient = ADAPTER_SCALE * jnp.einsum('fb,fd->bd', down_projected[:, narrow_rank_rows:], value_gradient, preferred_element_type=jnp.float32)
        middle_gradient = jnp.concatenate([jnp.dot(query_gradient, query_up_adapter.T, preferred_element_type=jnp.float32), jnp.dot(value_gradient, value_up_adapter.T, preferred_element_type=jnp.float32)], 1).astype(jnp.bfloat16)
        down_gradient = ADAPTER_SCALE * jnp.einsum('uh,ux->hx', normed_input, middle_gradient, preferred_element_type=jnp.float32)
        return (attended, down_gradient, query_up_gradient, value_up_gradient)
    attn_out, down_gradient, query_up_gradient, value_up_gradient = lax.map(one_sequence, (tokens, out_grad))
    down_gradient = lax.optimization_barrier(jnp.sum(down_gradient, axis=0))
    return (attn_out, down_gradient[:, :narrow_rank_rows], lax.optimization_barrier(jnp.sum(query_up_gradient, axis=0)), down_gradient[:, narrow_rank_rows:], lax.optimization_barrier(jnp.sum(value_up_gradient, axis=0)))
```

```python
import functools
import math

import jax
import jax.numpy as jnp
from jax import lax
from jax.experimental import pallas as pl
from jax.experimental.pallas import tpu as pltpu
from jax.sharding import PartitionSpec as P

HD = 128
QUERY_PER_KV = 8


EPSILON = 1e-05
ADAPTER_SCALE = 2.0
ROPE_BASE = 500000.0


def normalize(own_rows, norm_gain):
    widened = own_rows.astype(jnp.float32)
    mean_square = jnp.mean(widened * widened, axis=-1, keepdims=True)
    return (widened * lax.rsqrt(mean_square + EPSILON) * norm_gain).astype(jnp.bfloat16)


def rotary_tables(sequence_length):
    half_dim = HD // 2
    positions = jnp.arange(sequence_length, dtype=jnp.float32)[:, None]
    inv_freq = ROPE_BASE ** (-jnp.arange(half_dim, dtype=jnp.float32) / half_dim)
    angles = positions * inv_freq
    cosine, sine = jnp.cos(angles), jnp.sin(angles)
    return jnp.concatenate([cosine, cosine], 1), jnp.concatenate([-sine, sine], 1)


def dot(a, b, dims):
    return lax.dot_general(a, b, (dims, ((), ())), preferred_element_type=jnp.float32)


def attention_kernel(
    block, q_ref, k_ref, v_ref, dq_ref, dv_ref, qup_ref, vup_ref, cos_ref, sin_ref, g_ref,
    out_ref, gbq_ref, gbv_ref, midq_ref, midv_ref,
    keys, values, value_grad, query_grad,
):
    group, head = pl.program_id(0), pl.program_id(1)
    heads = pl.num_programs(1)
    length = q_ref.shape[0]
    scale = 1.0 / math.sqrt(HD)

    @pl.when(head == 0)
    def _():
        k = k_ref[...].astype(jnp.bfloat16).astype(jnp.float32)
        keys[...] = (k * cos_ref[...] + pltpu.roll(k, HD // 2, 1) * sin_ref[...]).astype(jnp.bfloat16)
        values[...] = (
            v_ref[...] + ADAPTER_SCALE * dot(dv_ref[...], vup_ref[...], ((1,), (0,)))
        ).astype(jnp.bfloat16)
        value_grad[...] = jnp.zeros_like(value_grad)

    @pl.when((head == 0) & (group == 0))
    def _():
        midq_ref[...] = jnp.zeros_like(midq_ref)
        midv_ref[...] = jnp.zeros_like(midv_ref)

    for start in range(0, length, block):
        rows = pl.ds(start, block)
        reach = start + block
        q = (
            q_ref[rows, :] + ADAPTER_SCALE * dot(dq_ref[rows, :], qup_ref[...], ((1,), (0,)))
        ).astype(jnp.bfloat16).astype(jnp.float32)
        cosine, sine = cos_ref[rows, :], sin_ref[rows, :]
        turned = (q * cosine + pltpu.roll(q, HD // 2, 1) * sine).astype(jnp.bfloat16)
        k, v, g = keys[pl.ds(0, reach), :], values[pl.ds(0, reach), :], g_ref[rows, :]
        scores = dot(turned, k, ((1,), (1,))) * scale
        row = lax.broadcasted_iota(jnp.int32, scores.shape, 0) + start
        col = lax.broadcasted_iota(jnp.int32, scores.shape, 1)
        scores = jnp.where(row >= col, scores, -1e30)
        weights = jnp.exp(scores - jnp.max(scores, axis=-1, keepdims=True))
        wide = weights * (1.0 / jnp.sum(weights, axis=-1, keepdims=True))
        probabilities = wide.astype(jnp.bfloat16)
        out_ref[rows, :] = dot(probabilities, v, ((1,), (0,))).astype(jnp.bfloat16)
        value_grad[pl.ds(0, reach), :] += dot(probabilities, g, ((0,), (0,)))
        prob_grad = dot(g, v, ((1,), (1,)))
        inner = jnp.sum(prob_grad * wide, axis=-1, keepdims=True)
        score_grad = (wide * (prob_grad - inner) * scale).astype(jnp.bfloat16)
        turned_grad = dot(score_grad, k, ((1,), (0,))).astype(jnp.bfloat16).astype(jnp.float32)
        query_grad[rows, :] = (
            turned_grad * cosine - pltpu.roll(turned_grad, HD // 2, 1) * sine
        ).astype(jnp.bfloat16)

    gq = query_grad[...]
    gbq_ref[...] = ADAPTER_SCALE * dot(dq_ref[...], gq, ((0,), (0,)))
    midq_ref[...] += dot(gq, qup_ref[...], ((1,), (1,)))

    @pl.when(head == heads - 1)
    def _():
        gv = value_grad[...].astype(jnp.bfloat16)
        gbv_ref[...] = ADAPTER_SCALE * dot(dv_ref[...], gv, ((0,), (0,)))
        midv_ref[...] += dot(gv, vup_ref[...], ((1,), (1,)))


def attention(projected, down_q, down_v, query_up, value_up, grad_rows):
    length, cols = projected.shape
    rank = down_q.shape[1]
    per = QUERY_PER_KV + 2
    groups = cols // (per * HD)
    block = 256 if length % 256 == 0 else length
    cosine, sine = rotary_tables(length)
    heads = groups * QUERY_PER_KV
    whole = lambda shape: pl.BlockSpec(shape, lambda g, h: (0, 0))
    column = lambda n, index: pl.BlockSpec((n, HD), lambda g, h: (0, index(g, h)))
    by_head = lambda g, h: g * QUERY_PER_KV + h
    return pl.pallas_call(
        functools.partial(attention_kernel, block),
        grid=(groups, QUERY_PER_KV),
        in_specs=[
            column(length, lambda g, h: g * per + h),
            column(length, lambda g, h: g * per + QUERY_PER_KV),
            column(length, lambda g, h: g * per + QUERY_PER_KV + 1),
            whole((length, rank)),
            whole((length, rank)),
            column(rank, by_head),
            column(rank, lambda g, h: g),
            whole((length, HD)),
            whole((length, HD)),
            column(length, by_head),
        ],
        out_specs=[
            column(length, by_head),
            column(rank, by_head),
            column(rank, lambda g, h: g),
            whole((length, rank)),
            whole((length, rank)),
        ],
        out_shape=[
            jax.ShapeDtypeStruct((length, heads * HD), jnp.bfloat16),
            jax.ShapeDtypeStruct((rank, heads * HD), jnp.float32),
            jax.ShapeDtypeStruct((rank, groups * HD), jnp.float32),
            jax.ShapeDtypeStruct((length, rank), jnp.float32),
            jax.ShapeDtypeStruct((length, rank), jnp.float32),
        ],
        scratch_shapes=[
            pltpu.VMEM((length, HD), jnp.bfloat16),
            pltpu.VMEM((length, HD), jnp.bfloat16),
            pltpu.VMEM((length, HD), jnp.float32),
            pltpu.VMEM((length, HD), jnp.bfloat16),
        ],
        compiler_params=pltpu.CompilerParams(
            dimension_semantics=("arbitrary", "arbitrary"), vmem_limit_bytes=48 * 2**20
        ),
        cost_estimate=pl.CostEstimate(
            flops=10 * heads * length * length * HD,
            bytes_accessed=length * cols * 4 + 2 * length * heads * HD * 2,
            transcendentals=heads * length * length,
        ),
        name="attention",
    )(projected, projected, projected, down_q, down_v, query_up, value_up, cosine, sine, grad_rows)


def local(count, tokens, norm_gain, w_qkv, a_query, query_up_adapter, a_value, value_up_adapter, out_grad):
    own = normalize(tokens[0], norm_gain)
    own_rows = own.shape[0]
    rank = a_query.shape[1]
    place = lax.axis_index("tensor")
    weights = lax.all_gather(w_qkv, ("dp", "fsdp"), axis=0, tiled=True)
    adapters = jnp.concatenate([a_query, a_value], 1)
    grad_rows = lax.all_to_all(out_grad[0], "tensor", split_axis=1, concat_axis=0, tiled=True)

    down_own = jnp.dot(own, adapters, preferred_element_type=jnp.float32).astype(jnp.bfloat16)
    down_projected = lax.all_gather(down_own, "tensor", axis=0, tiled=True)

    upward, downward = [], []
    up_block = down_block = own
    for step in range(1, count):
        if step > 1 and step == count - 1:
            up_block, down_block, weights = lax.optimization_barrier((up_block, down_block, weights))
            upward[-1], downward[-1] = up_block, down_block
        up_block = lax.ppermute(up_block, "tensor", [(i, i + 1) for i in range(step - 1, count - 1)])
        down_block = lax.ppermute(down_block, "tensor", [(i, i - 1) for i in range(1, count - step + 1)])
        upward.append(up_block)
        downward.append(down_block)
    blocks = [
        jnp.dot(rows, weights, preferred_element_type=jnp.float32)
        for rows in upward[::-1] + [own] + downward
    ]
    window = (count - 1 - place) * own_rows
    projected = lax.dynamic_slice_in_dim(jnp.concatenate(blocks, 0), window, count * own_rows, 0)
    attended, query_up_gradient, value_up_gradient, mid_query, mid_value = attention(
        projected, down_projected[:, :rank], down_projected[:, rank:],
        query_up_adapter, value_up_adapter, grad_rows,
    )
    out_rows = lax.all_to_all(attended, "tensor", split_axis=0, concat_axis=1, tiled=True)
    mid_own = lax.psum_scatter(
        jnp.concatenate([mid_query, mid_value], 1), "tensor", scatter_dimension=0, tiled=True
    ).astype(jnp.bfloat16)
    down_gradient = ADAPTER_SCALE * jnp.einsum(
        "uh,ux->xh", own, mid_own, preferred_element_type=jnp.float32
    )
    down_gradient = lax.psum(down_gradient, ("dp", "fsdp", "tensor")).T
    query_up_gradient, value_up_gradient = lax.psum(
        (query_up_gradient, value_up_gradient), ("dp", "fsdp")
    )
    return (
        out_rows[None],
        down_gradient[:, :rank],
        query_up_gradient,
        down_gradient[:, rank:],
        value_up_gradient,
    )


def solution(mesh):
    return jax.shard_map(
        functools.partial(local, mesh.shape["tensor"]),
        mesh=mesh,
        in_specs=(
            P(("dp", "fsdp"), "tensor", None),
            P(),
            P(("dp", "fsdp"), "tensor"),
            P(),
            P(None, "tensor"),
            P(),
            P(None, "tensor"),
            P(("dp", "fsdp"), "tensor", None),
        ),
        out_specs=(
            P(("dp", "fsdp"), "tensor", None),
            P(),
            P(None, "tensor"),
            P(),
            P(None, "tensor"),
        ),
        check_vma=False,
    )
```
